256 devices in a mesh: rep: 4 (over x, y), exp: 2 (over core), tp: 32 (over z).
Axes of the slice: x: 2, y: 2, z: 32, core: 2. Of those that a mesh axis runs over, the one named last changes fastest.
The devices are a block of a 4x8x32 slice.
Arguments:
- tokens: bfloat16 [2048, 4096], P(('rep', 'exp'), 'tp'), parts along dimension 0
- smooth_in: float32 [4096], P('tp'), may hold values from 0.5 to 2
- expert_ids: int32 [2048, 2], P(('rep', 'exp')), parts along dimension 0, may hold values from 0 to 3, as said below
- gate_fixed: int32 [2048, 2], P(('rep', 'exp')), parts along dimension 0, may hold values from 1 to 32767
- slots: int32 [2048, 2], P(('rep', 'exp')), parts along dimension 0, may hold values from 0 to 255, as said below
- w_gate: bfloat16 [4, 4096, 7168], P('exp', None, 'tp')
- w_up: bfloat16 [4, 4096, 7168], P('exp', None, 'tp')
- w_down: bfloat16 [4, 7168, 4096], P('exp', 'tp')
- gate_scale: float32 [4, 7168], P('exp', 'tp'), may hold values from 0.00010557433 to 0.0004222973
- up_scale: float32 [4, 7168], P('exp', 'tp'), may hold values from 0.00010557433 to 0.0004222973
- smooth_mid: float32 [4, 7168], P('exp', 'tp'), may hold values from 0.5 to 2
- down_scale: float32 [4, 4096], P('exp'), may hold values from 0.00015961338 to 0.0006384535
Outputs:
- moe_out: bfloat16 [2048, 4096], P(('rep', 'exp'), 'tp'), parts along dimension 0
The draws below stay inside these ranges and needn't reach their ends.
There are 4 independent parts, one for each index of `rep`. The reference program is written for one: setup_inputs(seed, part) draws one part's arguments, and reference() takes and returns one part's arrays. A program takes and returns all parts, laid end to end along the dimension named above; an argument that names none is the same for every part. Nothing has to cross between parts.
Inputs may be any that keep to these rules, and one draw needn't show every extreme that they name: `expert_ids`: the two experts of a token differ. Within one aligned block of 256 tokens (the tokens of one index of exp), the slots of the pairs that name one expert are distinct and run from 0 to their number less one. In every block some expert is named by 192 or more tokens.
All inputs are finite; a program needn't handle non-finite values.
Results may differ from the reference program's by a relative error of at most 0.006.
Values may be sent and summed in bfloat16 or wider, within the bound.
No kernel may reach another device: no remote copies, remote signals or barrier semaphores. Data moves between devices by JAX's collectives and lax.ppermute only.
A program may use at most 64 MiB of HBM per device.

```python
import math
import jax
import jax.numpy as jnp
from jax import lax

D = 4096
FF = 7168
TOP = 2
BLK = 256
EXPERTS = 4
CAP = 192
TOKENS = 512


def routing(key):
    routing_key = jax.random.fold_in(key, 11)
    subkeys = jax.random.split(routing_key, 7)
    blocks = TOKENS // BLK
    hot_expert = jax.random.randint(subkeys[0], (), 0, EXPERTS)
    priority = jax.random.randint(subkeys[1], (blocks, BLK), 0, 1 << 20) * BLK + jnp.arange(BLK, dtype=jnp.int32)[None, :]
    position = jnp.argsort(jnp.argsort(priority, axis=1, stable=True), axis=1, stable=True)
    coin_flip = jax.random.randint(subkeys[2], (blocks, BLK), 0, 2)
    with_hot = ((position < CAP) | (coin_flip == 1)).reshape(TOKENS)
    first_off = jax.random.randint(subkeys[3], (TOKENS,), 1, EXPERTS)
    second_off = 1 + (first_off - 1 + jax.random.randint(subkeys[4], (TOKENS,), 1, EXPERTS - 1)) % (EXPERTS - 1)
    other_a = (hot_expert + first_off) % EXPERTS
    other_b = (hot_expert + second_off) % EXPERTS
    pair_one = jnp.where(with_hot, hot_expert, other_b)
    pair_two = other_a
    order_flip = jax.random.randint(subkeys[5], (TOKENS,), 0, 2)
    first = jnp.where(order_flip == 1, pair_two, pair_one)
    second = jnp.where(order_flip == 1, pair_one, pair_two)
    expert_list = jnp.stack([first, second], axis=1).astype(jnp.int32)
    slot_priority = jax.random.randint(subkeys[6], (blocks, 2 * BLK), 0, 1 << 20) * (2 * BLK) + jnp.arange(2 * BLK, dtype=jnp.int32)[None, :]
    flat_ids = expert_list.reshape(blocks, 2 * BLK)
    same_expert = flat_ids[:, :, None] == flat_ids[:, None, :]
    earlier = slot_priority[:, None, :] < slot_priority[:, :, None]
    slot_list = jnp.sum((same_expert & earlier).astype(jnp.int32), axis=2).reshape(TOKENS, 2)
    return (expert_list, slot_list.astype(jnp.int32))


def draw_expert_ids(key, part):
    expert_list, slot_list = routing(key)
    return expert_list


def draw_slots(key, part):
    expert_list, slot_list = routing(key)
    return slot_list


def int_weights(key, shape):
    return jax.random.randint(key, shape, -127, 128).astype(jnp.float32).astype(jnp.bfloat16)


def draw_w_gate(key, part):
    return int_weights(jax.random.fold_in(key, 1), (EXPERTS, D, FF))


def draw_w_up(key, part):
    return int_weights(jax.random.fold_in(key, 2), (EXPERTS, D, FF))


def draw_w_down(key, part):
    return int_weights(jax.random.fold_in(key, 3), (EXPERTS, FF, D))


def draw_tokens(key, part):
    subkeys = jax.random.split(jax.random.fold_in(key, 4), 3)
    column_scale = jnp.exp(jax.random.uniform(subkeys[0], (D,), jnp.float32, math.log(0.3), math.log(3.0)))
    row_scale = jnp.exp(jax.random.uniform(subkeys[1], (TOKENS, 1), jnp.float32, math.log(0.5), math.log(2.0)))
    values = jax.random.normal(subkeys[2], (TOKENS, D), jnp.float32)
    return (values * column_scale[None, :] * row_scale).astype(jnp.bfloat16)


def touch_ends(entries, own_key, smallest, high):
    longest = entries.shape.index(max(entries.shape))
    spots = []
    for shift in (0, 1):
        where = [jax.random.randint(jax.random.fold_in(own_key, axis), (), 0, length) for axis, length in enumerate(entries.shape)]
        where[longest] = (where[longest] + shift) % entries.shape[longest]
        spots.append(tuple(where))
    return entries.at[spots[0]].set(smallest).at[spots[1]].set(high)


def levels(rng, extent, cuts, least, top_value):
    def one(dim, blocks):
        draws = jax.random.uniform(jax.random.fold_in(jax.random.fold_in(rng, 6), dim), (blocks,), jnp.float32, least / len(cuts), top_value / len(cuts))
        return jnp.repeat(jnp.exp(draws), extent[dim] // blocks).reshape((-1,) + (1,) * (len(extent) - dim - 1))

    level = one(*cuts[0])
    for cut in cuts[1:]:
        level = level * one(*cut)
    return level


def setup_inputs(seed: int = 0, part: int = 0) -> dict:
    key_list = jax.random.split(jax.random.key(seed), 13)
    part_keys = jax.random.split(jax.random.fold_in(key_list[12], part), 13)
    return {
        "tokens": draw_tokens(jax.random.fold_in(jax.random.fold_in(key_list[12], part), 71), part),
        "smooth_in": jnp.clip(jnp.exp(math.log(2.0) - 1.3862944 * jax.random.uniform(key_list[1], (D,), jnp.float32) ** levels(key_list[1], (D,), ((0, 32),), -0.2, 0.2)), 0.5, 2.0),
        "expert_ids": draw_expert_ids(jax.random.fold_in(jax.random.fold_in(key_list[12], part), 71), part),
        "gate_fixed": touch_ends(jax.random.randint(part_keys[3], (TOKENS, TOP), 1, 32768), jax.random.fold_in(part_keys[3], 1), 1, 32767).astype(jnp.int32),
        "slots": draw_slots(jax.random.fold_in(jax.random.fold_in(key_list[12], part), 71), part),
        "w_gate": draw_w_gate(jax.random.fold_in(key_list[12], 71), part),
        "w_up": draw_w_up(jax.random.fold_in(key_list[12], 71), part),
        "w_down": draw_w_down(jax.random.fold_in(key_list[12], 71), part),
        "gate_scale": jnp.clip(jnp.exp(math.log(0.0004222973) - 1.3862944 * jax.random.uniform(key_list[8], (EXPERTS, FF), jnp.float32) ** levels(key_list[8], (EXPERTS, FF), ((0, 2), (1, 32)), -0.2, 0.2)), 0.00010557433, 0.0004222973),
        "up_scale": jnp.clip(jnp.exp(math.log(0.0004222973) - 1.3862944 * jax.random.uniform(key_list[9], (EXPERTS, FF), jnp.float32) ** levels(key_list[9], (EXPERTS, FF), ((0, 2), (1, 32)), -0.2, 0.2)), 0.00010557433, 0.0004222973),
        "smooth_mid": jnp.clip(jnp.exp(math.log(2.0) - 1.3862944 * jax.random.uniform(key_list[10], (EXPERTS, FF), jnp.float32) ** levels(key_list[10], (EXPERTS, FF), ((0, 2), (1, 32)), -0.2, 0.2)), 0.5, 2.0),
        "down_scale": jnp.clip(jnp.exp(math.log(0.0006384535) - 1.3862944 * jax.random.uniform(key_list[11], (EXPERTS, D), jnp.float32) ** levels(key_list[11], (EXPERTS, D), ((0, 2),), -0.2, 0.2)), 0.00015961338, 0.0006384535),
    }


CLIP_RATIO = 0.35
EPSILON = 1e-6


def expert_rows(quantized, in_scale, weights_of):
    gate_e, up_e, down_e, gate_sc, up_sc, smooth_e, down_sc = weights_of
    gate_pre = jnp.dot(quantized, gate_e, preferred_element_type=jnp.float32) * in_scale[:, None] * gate_sc[None, :]
    up_pre = jnp.dot(quantized, up_e, preferred_element_type=jnp.float32) * in_scale[:, None] * up_sc[None, :]
    hidden = jax.nn.silu(gate_pre) * up_pre / smooth_e[None, :]
    mid_scale = CLIP_RATIO * (jnp.max(jnp.abs(hidden), axis=1) + EPSILON) / 127.0
    hidden_q = jnp.clip(hidden / mid_scale[:, None], -127.0, 127.0).astype(jnp.bfloat16)
    down_acc = jnp.dot(hidden_q, down_e, preferred_element_type=jnp.float32)
    return down_acc * mid_scale[:, None] * down_sc[None, :]


def reference(tokens, smooth_in, expert_ids, gate_fixed, slots, w_gate, w_up, w_down, gate_scale, up_scale, smooth_mid, down_scale):
    smoothed = tokens.astype(jnp.float32) / smooth_in[None, :]
    in_scale = CLIP_RATIO * (jnp.max(jnp.abs(smoothed), axis=1) + EPSILON) / 127.0
    quantized = jnp.clip(smoothed / in_scale[:, None], -127.0, 127.0).astype(jnp.bfloat16)
    gate_values = gate_fixed.astype(jnp.float32)
    weight = gate_values / jnp.sum(gate_values, axis=1, keepdims=True)
    pair_weight = jnp.where(slots < CAP, weight, jnp.zeros_like(weight))

    def add_expert(accumulated, expert_index):
        weights_of = (w_gate[expert_index], w_up[expert_index], w_down[expert_index],
                      gate_scale[expert_index], up_scale[expert_index], smooth_mid[expert_index], down_scale[expert_index])
        produced = expert_rows(quantized, in_scale, weights_of)
        share = jnp.sum(jnp.where(expert_ids == expert_index, pair_weight, jnp.zeros_like(pair_weight)), axis=1)
        return accumulated + produced * share[:, None], expert_index

    start_sum = jnp.zeros((TOKENS, D), jnp.float32)
    accumulated, unused = lax.scan(add_expert, start_sum, jnp.arange(EXPERTS, dtype=jnp.int32))
    return accumulated.astype(jnp.bfloat16)
```

```python
import functools

import jax
import jax.numpy as jnp
from jax import lax
from jax.experimental import pallas as pl
from jax.experimental.pallas import tpu as pltpu
from jax.sharding import PartitionSpec as P

CLIP_RATIO = 0.35
EPSILON = 1e-06
LANES = 128
PAD = 8

GATHER_BASE = (-12, -8, -4, 0, 4, 8, 12, 16)
SUM_BASE = (4, 8, 12, 0, -4, -8, -12, 16)
SUM_UP = tuple(o + 1 for o in SUM_BASE)
SUM_DOWN = tuple(o - 1 for o in SUM_BASE)
FIRST_UP = (6, 10, 14, 2)
FIRST_DOWN = (-2, -6, -10, -14)


def split_three(value):
    high = lax.reduce_precision(value, 8, 7)
    rest = value - high
    middle = lax.reduce_precision(rest, 8, 7)
    low = lax.reduce_precision(rest - middle, 8, 7)
    return high, middle, low


def to_partner(array):
    return lax.ppermute(array, "exp", [(0, 1), (1, 0)])


def shift(array, by):
    size = lax.axis_size("tp")
    return lax.ppermute(array, "tp", [(i, (i + by) % size) for i in range(size)])


def both_ways(up, down, by):
    return lax.optimization_barrier((shift(up, by), shift(down, -by)))


def gather_features(packed):
    far = lax.optimization_barrier(shift(packed, 16))
    two = jnp.stack([packed, far])
    below, above = both_ways(two, two, 4)
    below2, above2 = both_ways(below[0], above[0], 4)
    base = jnp.stack([above[1], below2, below[0], packed, above[0], above2, below[1], far])
    left, right = both_ways(base, base, 1)
    left2, right2 = both_ways(left[:4], right[3:7], 1)
    return (
        (base, GATHER_BASE),
        (left, tuple(o - 1 for o in GATHER_BASE)),
        (right, tuple(o + 1 for o in GATHER_BASE)),
        (left2, tuple(o - 2 for o in GATHER_BASE[:4])),
        (right2, tuple(o + 2 for o in GATHER_BASE[3:7])),
    )


def column_of(row):
    return jnp.transpose(jnp.broadcast_to(row, (LANES, row.shape[1])))


def row_of(column):
    return jnp.transpose(jnp.broadcast_to(column, (column.shape[0], LANES)))[0:1]


def quantize_kernel(offsets, n, me_ref, *refs):
    blocks, (q_ref, scale_ref) = refs[: len(offsets)], refs[len(offsets) :]
    rows = q_ref.shape[0]
    me = me_ref[0]

    def smoothed(ref, b):
        values = ref[b].astype(jnp.float32)
        factor = values[rows : rows + 1] + values[rows + 1 : rows + 2] + values[rows + 2 : rows + 3]
        return values[:rows] * (1.0 / factor)

    peak = jnp.zeros((rows, LANES), jnp.float32)
    for ref, block_offsets in zip(blocks, offsets):
        for b in range(len(block_offsets)):
            peak = jnp.maximum(peak, jnp.abs(smoothed(ref, b)))
    scale = CLIP_RATIO * (jnp.max(peak, axis=1, keepdims=True) + EPSILON) / 127.0
    scale_ref[...] = jnp.broadcast_to(row_of(scale), scale_ref.shape)
    inverse = 1.0 / scale
    for ref, block_offsets in zip(blocks, offsets):
        for b, offset in enumerate(block_offsets):
            start = pl.multiple_of(lax.rem(me + (offset + n), n) * LANES, LANES)
            value = jnp.clip(smoothed(ref, b) * inverse, -127.0, 127.0)
            q_ref[:, pl.ds(start, LANES)] = value.astype(jnp.bfloat16)


def quantize(me, gathered, rows, n):
    arrays = [a for a, _ in gathered]
    offsets = [o for _, o in gathered]
    vmem = pl.BlockSpec(memory_space=pltpu.VMEM)
    return pl.pallas_call(
        functools.partial(quantize_kernel, offsets, n),
        out_shape=(
            jax.ShapeDtypeStruct((rows, n * LANES), jnp.bfloat16),
            jax.ShapeDtypeStruct((8, rows), jnp.float32),
        ),
        in_specs=[pl.BlockSpec(memory_space=pltpu.SMEM)] + [vmem] * len(arrays),
        out_specs=(vmem, vmem),
        compiler_params=pltpu.CompilerParams(vmem_limit_bytes=24 << 20),
        cost_estimate=pl.CostEstimate(flops=20_000_000, bytes_accessed=4 << 20, transcendentals=0),
        name="quantize",
    )(me, *arrays)


def hidden_kernel(q_ref, scale_ref, gate_ref, up_ref, gs_ref, us_ref, sm_ref, hidden_ref, peak_ref):
    scale = column_of(scale_ref[...])[:, 0:1]
    contract = (((1,), (1,)), ((), ()))
    gate = lax.dot_general(q_ref[...], gate_ref[0], contract, preferred_element_type=jnp.float32)
    up = lax.dot_general(q_ref[...], up_ref[0], contract, preferred_element_type=jnp.float32)
    gate = gate * scale * gs_ref[0]
    up = up * scale * us_ref[0]
    hidden = gate * (1.0 / (1.0 + jnp.exp(-gate))) * up * (1.0 / sm_ref[0])
    hidden_ref[0] = hidden
    peak_ref[0] = row_of(jnp.max(jnp.abs(hidden), axis=1, keepdims=True))


def hidden_of(q, scale, gate_t, up_t, gate_scale, up_scale, smooth_mid):
    experts, units, depth = gate_t.shape
    rows = q.shape[0]
    weights = pl.BlockSpec((1, units, depth), lambda e: (e, 0, 0))
    channel = pl.BlockSpec((1, 1, units), lambda e: (e, 0, 0))
    return pl.pallas_call(
        hidden_kernel,
        grid=(experts,),
        out_shape=(
            jax.ShapeDtypeStruct((experts, rows, units), jnp.float32),
            jax.ShapeDtypeStruct((experts, 1, rows), jnp.float32),
        ),
        in_specs=[
            pl.BlockSpec((rows, depth), lambda e: (0, 0)),
            pl.BlockSpec((1, rows), lambda e: (0, 0)),
            weights, weights, channel, channel, channel,
        ],
        out_specs=(
            pl.BlockSpec((1, rows, units), lambda e: (e, 0, 0)),
            pl.BlockSpec((1, 1, rows), lambda e: (e, 0, 0)),
        ),
        compiler_params=pltpu.CompilerParams(vmem_limit_bytes=24 << 20),
        cost_estimate=pl.CostEstimate(
            flops=4 * experts * rows * units * depth, bytes_accessed=10 << 20, transcendentals=0
        ),
        name="hidden",
    )(q, scale, gate_t, up_t, gate_scale[:, None], up_scale[:, None], smooth_mid[:, None])


def down_kernel(outputs, n, me_ref, hidden_ref, peak_ref, share_ref, down_ref, ds_ref, *refs):
    out_refs = refs[-len(outputs) :]
    from_ref = refs[0] if len(refs) > len(outputs) else None
    experts = hidden_ref.shape[0]
    me = me_ref[0]
    quantized, coefficient = [], []
    for e in range(experts):
        scale = CLIP_RATIO * (peak_ref[e : e + 1] + EPSILON) / 127.0
        inverse = column_of(1.0 / scale)[:, 0:1]
        quantized.append(jnp.clip(hidden_ref[e] * inverse, -127.0, 127.0).astype(jnp.bfloat16))
        coefficient.append(column_of(scale * share_ref[e : e + 1]))
    place = 0
    for offsets, ref in zip(outputs, out_refs):
        for b, offset in enumerate(offsets):
            start = pl.multiple_of(lax.rem(me + (offset + n), n) * LANES, LANES)
            total = None
            for e in range(experts):
                acc = jnp.dot(
                    quantized[e], down_ref[e, :, pl.ds(start, LANES)], preferred_element_type=jnp.float32
                )
                term = acc * coefficient[e] * ds_ref[e : e + 1, pl.ds(start, LANES)]
                total = term if total is None else total + term
            if from_ref is not None:
                total = total + from_ref[place].astype(jnp.float32)
            ref[b] = total.astype(ref.dtype)
            place += 1


def down(me, hidden, peaks, share, w_down, down_scale, outputs, types, arrived, n):
    rows, units = hidden.shape[1:]
    vmem = pl.BlockSpec(memory_space=pltpu.VMEM)
    extra = [] if arrived is None else [arrived]
    return pl.pallas_call(
        functools.partial(down_kernel, outputs, n),
        out_shape=tuple(
            jax.ShapeDtypeStruct((len(o), rows, LANES), t) for o, t in zip(outputs, types)
        ),
        in_specs=[pl.BlockSpec(memory_space=pltpu.SMEM)] + [vmem] * (5 + len(extra)),
        out_specs=tuple(vmem for _ in outputs),
        compiler_params=pltpu.CompilerParams(vmem_limit_bytes=32 << 20),
        cost_estimate=pl.CostEstimate(
            flops=4 * rows * units * n * LANES, bytes_accessed=8 << 20, transcendentals=0
        ),
        name="down",
    )(me, hidden, peaks, share, w_down, down_scale, *extra)


def peaks_of_all(peaks):
    size = lax.axis_size("tp")
    near = [list(range(i, i + 4)) for i in range(0, size, 4)]
    far = [list(range(i, size, 4)) for i in range(4)]
    for groups in (near, far):
        copies = jnp.broadcast_to(peaks[None], (len(groups[0]), *peaks.shape))
        peaks = lax.all_to_all(copies, "tp", 0, 0, axis_index_groups=groups, tiled=True).max(axis=0)
        peaks = lax.optimization_barrier(peaks)
    return peaks


def sum_over_tp(first_up, first_down, up, down_, base):
    def wide(a):
        return a.astype(jnp.float32)

    def sent(a):
        return a.astype(jnp.bfloat16)

    u, v = both_ways(first_up, first_down, 1)
    up = jnp.concatenate([up[:4] + wide(u), up[4:]])
    down_ = jnp.concatenate([down_[:3], down_[3:7] + wide(v), down_[7:]])
    u, v = both_ways(sent(up), sent(down_), 1)
    base = base + wide(u) + wide(v)
    u, v = both_ways(sent(base[1]), sent(base[5]), 4)
    plus, minus = base[0] + wide(u), base[4] + wide(v)
    u, v = both_ways(sent(jnp.stack([plus, base[6]])), sent(jnp.stack([minus, base[2]])), 4)
    near = base[3] + wide(u[0]) + wide(v[0])
    far = base[7] + wide(u[1]) + wide(v[1])
    return (near + wide(shift(sent(far), 16))).astype(jnp.bfloat16)


def per_device(
    tokens,
    smooth_in,
    expert_ids,
    gate_fixed,
    slots,
    w_gate,
    w_up,
    w_down,
    gate_scale,
    up_scale,
    smooth_mid,
    down_scale,
):
    local_experts = w_gate.shape[0]
    rows = tokens.shape[0]
    capacity = 3 * rows // 4
    group = lax.axis_index("exp")
    n = lax.axis_size("tp")
    assert n == 32 and tokens.shape[1] == LANES
    me = lax.axis_index("tp").astype(jnp.int32).reshape(1)

    parts = jnp.stack(split_three(smooth_in))
    parts = jnp.concatenate([parts, jnp.zeros((PAD - 3, LANES), parts.dtype)])
    packed = jnp.concatenate([tokens, parts.astype(jnp.bfloat16)])
    q, scale = quantize(me, gather_features(packed), rows, n)

    gate_values = gate_fixed.astype(jnp.float32)
    weight = gate_values / jnp.sum(gate_values, axis=1, keepdims=True)
    pair_weight = jnp.where(slots < capacity, weight, 0.0)

    def shares_of(which):
        experts = which * local_experts + jnp.arange(local_experts, dtype=jnp.int32)
        hit = expert_ids[:, :, None] == experts[None, None, :]
        return jnp.sum(jnp.where(hit, pair_weight[:, :, None], 0.0), axis=1).T

    share = shares_of(group)
    notes = jnp.concatenate([shares_of(1 - group), scale[: 8 - local_experts]])
    other_q = to_partner(q)
    other_notes = to_partner(notes)
    other_share, other_scale = other_notes[:local_experts], other_notes[local_experts : local_experts + 1]

    weights = (
        jnp.swapaxes(w_gate, 1, 2), jnp.swapaxes(w_up, 1, 2), gate_scale, up_scale, smooth_mid,
    )
    hidden, peak = hidden_of(q, scale[:1], *weights)
    other_hidden, other_peak = hidden_of(other_q, other_scale, *weights)
    peaks = peaks_of_all(jnp.concatenate([peak[:, 0], other_peak[:, 0]]))

    outputs = (FIRST_UP, FIRST_DOWN, SUM_UP, SUM_DOWN, SUM_BASE)
    order = (sum(outputs, ()),)
    (other_part,) = down(
        me, other_hidden, peaks[local_experts:], other_share, w_down, down_scale,
        order, (jnp.bfloat16,), None, n,
    )
    arrived = to_partner(other_part)
    types = (jnp.bfloat16, jnp.bfloat16, jnp.float32, jnp.float32, jnp.float32)
    partial = down(
        me, hidden, peaks[:local_experts], share, w_down, down_scale, outputs, types, arrived, n
    )
    return sum_over_tp(*partial)


def solution(mesh):
    in_specs = (
        P(("rep", "exp"), "tp"),
        P("tp"),
        P(("rep", "exp"), None),
        P(("rep", "exp"), None),
        P(("rep", "exp"), None),
        P("exp", None, "tp"),
        P("exp", None, "tp"),
        P("exp", "tp", None),
        P("exp", "tp"),
        P("exp", "tp"),
        P("exp", "tp"),
        P("exp", None),
    )
    out_specs = P(("rep", "exp"), "tp")
    return jax.shard_map(
        per_device, mesh=mesh, in_specs=in_specs, out_specs=out_specs, check_vma=False
    )
```

```python
import functools

import jax
import jax.numpy as jnp
from jax import lax
from jax.experimental import pallas as pl
from jax.experimental.pallas import tpu as pltpu
from jax.sharding import PartitionSpec as P

CLIP_RATIO = 0.35
EPSILON = 1e-06
LANES = 128
PAD = 8

SUM_BASE = tuple(range(-15, 16, 3))
SUM_UP = tuple(o + 1 for o in SUM_BASE)
SUM_DOWN = tuple(o - 1 for o in SUM_BASE[1:])
STRIDE = 4


def split_three(value):
    high = lax.reduce_precision(value, 8, 7)
    rest = value - high
    middle = lax.reduce_precision(rest, 8, 7)
    low = lax.reduce_precision(rest - middle, 8, 7)
    return high, middle, low


def to_partner(array):
    return lax.ppermute(array, "exp", [(0, 1), (1, 0)])


def shift(array, by):
    size = lax.axis_size("tp")
    return lax.ppermute(array, "tp", [(i, (i + by) % size) for i in range(size)])


def both_ways(up, down, by):
    return lax.optimization_barrier((shift(up, by), shift(down, -by)))


def strided_groups(size):
    return [list(range(i, size, STRIDE)) for i in range(STRIDE)]


def gather_features(packed):
    groups = strided_groups(lax.axis_size("tp"))
    count = len(groups[0])
    base = lax.all_gather(packed, "tp", axis=0, axis_index_groups=groups)
    base = lax.optimization_barrier(base)
    left, right = both_ways(base, base, 1)
    left2, right2 = both_ways(left[: count // 2], right[count // 2 :], 1)
    return ((base, 0, 0), (left, -1, 0), (right, 1, 0), (left2, -2, 0), (right2, 2, count // 2))


def column_of(row):
    return jnp.transpose(jnp.broadcast_to(row, (LANES, row.shape[1])))


def row_of(column):
    return jnp.transpose(jnp.broadcast_to(column, (column.shape[0], LANES)))[0:1]


def quantize_kernel(places, n, me_ref, *refs):
    blocks, (q_ref, scale_ref) = refs[: len(places)], refs[len(places) :]
    rows = q_ref.shape[0]
    me = me_ref[0]

    def smoothed(ref, b):
        values = ref[b].astype(jnp.float32)
        factor = values[rows : rows + 1] + values[rows + 1 : rows + 2] + values[rows + 2 : rows + 3]
        return values[:rows] * (1.0 / factor)

    peak = jnp.zeros((rows, LANES), jnp.float32)
    for ref in blocks:
        for b in range(ref.shape[0]):
            peak = jnp.maximum(peak, jnp.abs(smoothed(ref, b)))
    scale = CLIP_RATIO * (jnp.max(peak, axis=1, keepdims=True) + EPSILON) / 127.0
    scale_ref[...] = jnp.broadcast_to(row_of(scale), scale_ref.shape)
    inverse = 1.0 / scale
    for ref, (step, first) in zip(blocks, places):
        column = lax.rem(me + (step + n), STRIDE)
        for b in range(ref.shape[0]):
            start = pl.multiple_of((column + STRIDE * (first + b)) * LANES, LANES)
            value = jnp.clip(smoothed(ref, b) * inverse, -127.0, 127.0)
            q_ref[:, pl.ds(start, LANES)] = value.astype(jnp.bfloat16)


def quantize(me, gathered, rows, n):
    arrays = [array for array, _, _ in gathered]
    places = [(step, first) for _, step, first in gathered]
    vmem = pl.BlockSpec(memory_space=pltpu.VMEM)
    return pl.pallas_call(
        functools.partial(quantize_kernel, places, n),
        out_shape=(
            jax.ShapeDtypeStruct((rows, n * LANES), jnp.bfloat16),
            jax.ShapeDtypeStruct((8, rows), jnp.float32),
        ),
        in_specs=[pl.BlockSpec(memory_space=pltpu.SMEM)] + [vmem] * len(arrays),
        out_specs=(vmem, vmem),
        compiler_params=pltpu.CompilerParams(vmem_limit_bytes=24 << 20),
        cost_estimate=pl.CostEstimate(flops=20_000_000, bytes_accessed=4 << 20, transcendentals=0),
        name="quantize",
    )(me, *arrays)


def hidden_kernel(q_ref, scale_ref, gate_ref, up_ref, gs_ref, us_ref, sm_ref, hidden_ref, peak_ref):
    scale = column_of(scale_ref[...])[:, 0:1]
    contract = (((1,), (1,)), ((), ()))
    gate = lax.dot_general(q_ref[...], gate_ref[0], contract, preferred_element_type=jnp.float32)
    up = lax.dot_general(q_ref[...], up_ref[0], contract, preferred_element_type=jnp.float32)
    gate = gate * scale * gs_ref[0]
    up = up * scale * us_ref[0]
    hidden = gate * (1.0 / (1.0 + jnp.exp(-gate))) * up * (1.0 / sm_ref[0])
    hidden_ref[0] = hidden
    peak_ref[0] = row_of(jnp.max(jnp.abs(hidden), axis=1, keepdims=True))


def hidden_of(q, scale, gate_t, up_t, gate_scale, up_scale, smooth_mid):
    experts, units, depth = gate_t.shape
    rows = q.shape[0]
    weights = pl.BlockSpec((1, units, depth), lambda e: (e, 0, 0))
    channel = pl.BlockSpec((1, 1, units), lambda e: (e, 0, 0))
    return pl.pallas_call(
        hidden_kernel,
        grid=(experts,),
        out_shape=(
            jax.ShapeDtypeStruct((experts, rows, units), jnp.float32),
            jax.ShapeDtypeStruct((experts, 1, rows), jnp.float32),
        ),
        in_specs=[
            pl.BlockSpec((rows, depth), lambda e: (0, 0)),
            pl.BlockSpec((1, rows), lambda e: (0, 0)),
            weights, weights, channel, channel, channel,
        ],
        out_specs=(
            pl.BlockSpec((1, rows, units), lambda e: (e, 0, 0)),
            pl.BlockSpec((1, 1, rows), lambda e: (e, 0, 0)),
        ),
        compiler_params=pltpu.CompilerParams(vmem_limit_bytes=24 << 20),
        cost_estimate=pl.CostEstimate(
            flops=4 * experts * rows * units * depth, bytes_accessed=10 << 20, transcendentals=0
        ),
        name="hidden",
    )(q, scale, gate_t, up_t, gate_scale[:, None], up_scale[:, None], smooth_mid[:, None])


def down_kernel(outputs, n, me_ref, hidden_ref, peak_ref, share_ref, down_ref, ds_ref, *refs):
    out_refs = refs[-len(outputs) :]
    from_ref = refs[0] if len(refs) > len(outputs) else None
    experts = hidden_ref.shape[0]
    me = me_ref[0]
    quantized, coefficient = [], []
    for e in range(experts):
        scale = CLIP_RATIO * (peak_ref[e : e + 1] + EPSILON) / 127.0
        inverse = column_of(1.0 / scale)[:, 0:1]
        quantized.append(jnp.clip(hidden_ref[e] * inverse, -127.0, 127.0).astype(jnp.bfloat16))
        coefficient.append(column_of(scale * share_ref[e : e + 1]))
    place = 0
    for offsets, ref in zip(outputs, out_refs):
        for b, offset in enumerate(offsets):
            start = pl.multiple_of(lax.rem(me + (offset + n), n) * LANES, LANES)
            total = None
            for e in range(experts):
                acc = jnp.dot(
                    quantized[e], down_ref[e, :, pl.ds(start, LANES)], preferred_element_type=jnp.float32
                )
                term = acc * coefficient[e] * ds_ref[e : e + 1, pl.ds(start, LANES)]
                total = term if total is None else total + term
            if from_ref is not None:
                total = total + from_ref[place].astype(jnp.float32)
            ref[b] = total.astype(ref.dtype)
            place += 1


def down(me, hidden, peaks, share, w_down, down_scale, outputs, types, arrived, n):
    rows, units = hidden.shape[1:]
    vmem = pl.BlockSpec(memory_space=pltpu.VMEM)
    extra = [] if arrived is None else [arrived]
    return pl.pallas_call(
        functools.partial(down_kernel, outputs, n),
        out_shape=tuple(
            jax.ShapeDtypeStruct((len(o), rows, LANES), t) for o, t in zip(outputs, types)
        ),
        in_specs=[pl.BlockSpec(memory_space=pltpu.SMEM)] + [vmem] * (5 + len(extra)),
        out_specs=tuple(vmem for _ in outputs),
        compiler_params=pltpu.CompilerParams(vmem_limit_bytes=32 << 20),
        cost_estimate=pl.CostEstimate(
            flops=4 * rows * units * n * LANES, bytes_accessed=8 << 20, transcendentals=0
        ),
        name="down",
    )(me, hidden, peaks, share, w_down, down_scale, *extra)


def peaks_of_all(peaks):
    size = lax.axis_size("tp")
    near = [list(range(i, i + STRIDE)) for i in range(0, size, STRIDE)]
    copies = jnp.broadcast_to(peaks[None], (STRIDE, *peaks.shape))
    peaks = lax.all_to_all(copies, "tp", 0, 0, axis_index_groups=near, tiled=True).max(axis=0)
    return lax.pmax(lax.optimization_barrier(peaks), "tp", axis_index_groups=strided_groups(size))


def sum_over_tp(up, down_, base):
    def wide(a):
        return a.astype(jnp.float32)

    def sent(a):
        return a.astype(jnp.bfloat16)

    u, v = both_ways(up, down_, 1)
    base = jnp.concatenate([base[:1] + wide(u[:1]), base[1:] + wide(u[1:]) + wide(v)])
    last, middle = base.shape[0] - 1, base.shape[0] // 2
    plus, minus = base[last], base[0]
    for i in range(1, middle):
        u, v = both_ways(sent(plus), sent(minus), 3)
        plus, minus = base[last - i] + wide(u), base[i] + wide(v)
    u, v = both_ways(sent(plus), sent(minus), 3)
    return (base[middle] + wide(u) + wide(v)).astype(jnp.bfloat16)


def per_device(
    tokens,
    smooth_in,
    expert_ids,
    gate_fixed,
    slots,
    w_gate,
    w_up,
    w_down,
    gate_scale,
    up_scale,
    smooth_mid,
    down_scale,
):
    local_experts = w_gate.shape[0]
    rows = tokens.shape[0]
    capacity = 3 * rows // 4
    group = lax.axis_index("exp")
    n = lax.axis_size("tp")
    assert n == 32 and tokens.shape[1] == LANES
    me = lax.axis_index("tp").astype(jnp.int32).reshape(1)

    parts = jnp.stack(split_three(smooth_in))
    parts = jnp.concatenate([parts, jnp.zeros((PAD - 3, LANES), parts.dtype)])
    packed = jnp.concatenate([tokens, parts.astype(jnp.bfloat16)])
    q, scale = quantize(me, gather_features(packed), rows, n)

    gate_values = gate_fixed.astype(jnp.float32)
    weight = gate_values / jnp.sum(gate_values, axis=1, keepdims=True)
    pair_weight = jnp.where(slots < capacity, weight, 0.0)

    def shares_of(which):
        experts = which * local_experts + jnp.arange(local_experts, dtype=jnp.int32)
        hit = expert_ids[:, :, None] == experts[None, None, :]
        return jnp.sum(jnp.where(hit, pair_weight[:, :, None], 0.0), axis=1).T

    share = shares_of(group)
    notes = jnp.concatenate([shares_of(1 - group), scale[: 8 - local_experts]])
    other_q = to_partner(q)
    other_notes = to_partner(notes)
    other_share, other_scale = other_notes[:local_experts], other_notes[local_experts : local_experts + 1]

    weights = (
        jnp.swapaxes(w_gate, 1, 2), jnp.swapaxes(w_up, 1, 2), gate_scale, up_scale, smooth_mid,
    )
    hidden, peak = hidden_of(q, scale[:1], *weights)
    other_hidden, other_peak = hidden_of(other_q, other_scale, *weights)
    peaks = peaks_of_all(jnp.concatenate([peak[:, 0], other_peak[:, 0]]))

    outputs = (SUM_UP, SUM_DOWN, SUM_BASE)
    order = (sum(outputs, ()),)
    (other_part,) = down(
        me, other_hidden, peaks[local_experts:], other_share, w_down, down_scale,
        order, (jnp.bfloat16,), None, n,
    )
    arrived = to_partner(other_part)
    types = (jnp.bfloat16, jnp.bfloat16, jnp.float32)
    partial = down(
        me, hidden, peaks[:local_experts], share, w_down, down_scale, outputs, types, arrived, n
    )
    return sum_over_tp(*partial)


def solution(mesh):
    in_specs = (
        P(("rep", "exp"), "tp"),
        P("tp"),
        P(("rep", "exp"), None),
        P(("rep", "exp"), None),
        P(("rep", "exp"), None),
        P("exp", None, "tp"),
        P("exp", None, "tp"),
        P("exp", "tp", None),
        P("exp", "tp"),
        P("exp", "tp"),
        P("exp", "tp"),
        P("exp", None),
    )
    out_specs = P(("rep", "exp"), "tp")
    return jax.shard_map(
        per_device, mesh=mesh, in_specs=in_specs, out_specs=out_specs, check_vma=False
    )
```

```python
import functools

import jax
import jax.numpy as jnp
from jax import lax
from jax.experimental import pallas as pl
from jax.experimental.pallas import tpu as pltpu
from jax.sharding import PartitionSpec as P

CLIP_RATIO = 0.35
EPSILON = 1e-06
LANES = 128
PAD = 8

SUM_BASE = (-15, 15, -12, 12, -9, 9, -6, 6, -3, 3, 0)
OUTER = 4
SUM_UP = tuple(o + 1 for o in SUM_BASE)
SUM_DOWN = tuple(o - 1 for o in SUM_BASE[1:])
STRIDE = 4

PIECES = 2


def pack_kernel(tokens_ref, smooth_ref, packed_ref):
    rows = tokens_ref.shape[0]
    value = jnp.broadcast_to(smooth_ref[...], (PAD, LANES))
    high = value.astype(jnp.bfloat16).astype(jnp.float32)
    middle = (value - high).astype(jnp.bfloat16).astype(jnp.float32)
    low = value - high - middle
    row = lax.broadcasted_iota(jnp.int32, (PAD, LANES), 0)
    part = jnp.where(row == 0, high, jnp.where(row == 1, middle, low))
    packed_ref[:rows] = tokens_ref[...]
    packed_ref[rows:] = part.astype(jnp.bfloat16)


def pack(tokens, smooth_in):
    vmem = pl.BlockSpec(memory_space=pltpu.VMEM)
    return pl.pallas_call(
        pack_kernel,
        out_shape=jax.ShapeDtypeStruct((tokens.shape[0] + PAD, LANES), jnp.bfloat16),
        in_specs=[vmem, vmem],
        out_specs=vmem,
        name="pack",
    )(tokens, smooth_in[None])


def to_partner(array):
    return lax.ppermute(array, "exp", [(0, 1), (1, 0)])


def shift(array, by):
    size = lax.axis_size("tp")
    return lax.ppermute(array, "tp", [(i, (i + by) % size) for i in range(size)])


def both_ways(up, down, by):
    return lax.optimization_barrier((shift(up, by), shift(down, -by)))


def strided_groups(size):
    return [list(range(i, size, STRIDE)) for i in range(STRIDE)]


def gather_features(packed):
    groups = strided_groups(lax.axis_size("tp"))
    count = len(groups[0])
    base = lax.all_gather(packed, "tp", axis=0, axis_index_groups=groups)
    base = lax.optimization_barrier(base)
    left, right = both_ways(base, base, 1)
    left2, right2 = both_ways(left[: count // 2], right[count // 2 :], 1)
    return ((base, 0, 0), (left, -1, 0), (right, 1, 0), (left2, -2, 0), (right2, 2, count // 2))


def column_of(row):
    return jnp.transpose(jnp.broadcast_to(row, (LANES, row.shape[1])))


def row_of(column):
    return jnp.transpose(jnp.broadcast_to(column, (column.shape[0], LANES)))[0:1]


def quantize_kernel(places, n, me_ref, *refs):
    blocks, (q_ref, scale_ref) = refs[: len(places)], refs[len(places) :]
    rows = q_ref.shape[0]
    me = me_ref[0]

    def smoothed(ref, b):
        values = ref[b].astype(jnp.float32)
        factor = values[rows : rows + 1] + values[rows + 1 : rows + 2] + values[rows + 2 : rows + 3]
        return values[:rows] * (1.0 / factor)

    peak = jnp.zeros((rows, LANES), jnp.float32)
    for ref in blocks:
        for b in range(ref.shape[0]):
            peak = jnp.maximum(peak, jnp.abs(smoothed(ref, b)))
    scale = CLIP_RATIO * (jnp.max(peak, axis=1, keepdims=True) + EPSILON) / 127.0
    scale_ref[...] = jnp.broadcast_to(row_of(scale), scale_ref.shape)
    inverse = 1.0 / scale
    for ref, (step, first) in zip(blocks, places):
        column = lax.rem(me + (step + n), STRIDE)
        for b in range(ref.shape[0]):
            start = pl.multiple_of((column + STRIDE * (first + b)) * LANES, LANES)
            value = jnp.clip(smoothed(ref, b) * inverse, -127.0, 127.0)
            q_ref[:, pl.ds(start, LANES)] = value.astype(jnp.bfloat16)


def quantize(me, gathered, rows, n):
    arrays = [array for array, _, _ in gathered]
    places = [(step, first) for _, step, first in gathered]
    vmem = pl.BlockSpec(memory_space=pltpu.VMEM)
    return pl.pallas_call(
        functools.partial(quantize_kernel, places, n),
        out_shape=(
            jax.ShapeDtypeStruct((rows, n * LANES), jnp.bfloat16),
            jax.ShapeDtypeStruct((8, rows), jnp.float32),
        ),
        in_specs=[pl.BlockSpec(memory_space=pltpu.SMEM)] + [vmem] * len(arrays),
        out_specs=(vmem, vmem),
        compiler_params=pltpu.CompilerParams(vmem_limit_bytes=24 << 20),
        cost_estimate=pl.CostEstimate(flops=20_000_000, bytes_accessed=4 << 20, transcendentals=0),
        name="quantize",
    )(me, *arrays)


def hidden_kernel(
    q_ref, scale_ref, gs_ref, us_ref, sm_ref, gate_hbm, up_hbm, hidden_ref, peak_ref, gate_ref, up_ref, sems
):
    experts, _, depth = gate_ref.shape
    piece = depth // PIECES
    pairs = ((gate_hbm, gate_ref), (up_hbm, up_ref))

    def copy(e, c, w):
        part = pl.ds(c * piece, piece)
        source, target = pairs[w]
        return pltpu.make_async_copy(source.at[e, :, part], target.at[e, :, part], sems.at[e, c, w])

    for e in range(experts):
        for c in range(PIECES):
            for w in range(2):
                copy(e, c, w).start()
    scale = column_of(scale_ref[...])[:, 0:1]
    contract = (((1,), (1,)), ((), ()))
    for e in range(experts):
        totals = [None, None]
        for c in range(PIECES):
            part = slice(c * piece, (c + 1) * piece)
            for w in range(2):
                copy(e, c, w).wait()
                term = lax.dot_general(
                    q_ref[:, part], pairs[w][1][e, :, part], contract, preferred_element_type=jnp.float32
                )
                totals[w] = term if totals[w] is None else totals[w] + term
        gate = totals[0] * scale * gs_ref[e]
        up = totals[1] * scale * us_ref[e]
        hidden = gate * (1.0 / (1.0 + jnp.exp(-gate))) * up * (1.0 / sm_ref[e])
        hidden_ref[e] = hidden
        peak_ref[e] = row_of(jnp.max(jnp.abs(hidden), axis=1, keepdims=True))


def hidden_of(q, scale, gate_t, up_t, gate_scale, up_scale, smooth_mid):
    experts, units, depth = gate_t.shape
    rows = q.shape[0]
    vmem = pl.BlockSpec(memory_space=pltpu.VMEM)
    hbm = pl.BlockSpec(memory_space=pltpu.HBM)
    return pl.pallas_call(
        hidden_kernel,
        out_shape=(
            jax.ShapeDtypeStruct((experts, rows, units), jnp.float32),
            jax.ShapeDtypeStruct((experts, 1, rows), jnp.float32),
        ),
        in_specs=[vmem] * 5 + [hbm, hbm],
        out_specs=(vmem, vmem),
        scratch_shapes=[
            pltpu.VMEM(gate_t.shape, gate_t.dtype),
            pltpu.VMEM(up_t.shape, up_t.dtype),
            pltpu.SemaphoreType.DMA((experts, PIECES, 2)),
        ],
        compiler_params=pltpu.CompilerParams(vmem_limit_bytes=24 << 20),
        cost_estimate=pl.CostEstimate(
            flops=4 * experts * rows * units * depth, bytes_accessed=10 << 20, transcendentals=0
        ),
        name="hidden",
    )(
        q, scale, gate_scale[:, None], up_scale[:, None], smooth_mid[:, None],
        pltpu.with_memory_space_constraint(gate_t, pltpu.HBM),
        pltpu.with_memory_space_constraint(up_t, pltpu.HBM),
    )


def down_kernel(outputs, n, me_ref, hidden_ref, peak_ref, share_ref, ds_ref, down_hbm, *refs):
    weights, sems = refs[-2:]
    out_refs = refs[-2 - len(outputs) : -2]
    from_ref = refs[0] if len(refs) > len(outputs) + 2 else None
    experts = hidden_ref.shape[0]
    me = me_ref[0]
    order = sum(outputs, ())

    def columns(place):
        start = lax.rem(me + (order[place] + n), n) * LANES
        return pl.ds(pl.multiple_of(start, LANES), LANES)

    def copy(place):
        return pltpu.make_async_copy(down_hbm.at[:, :, columns(place)], weights.at[place], sems.at[place])

    for place in range(len(order)):
        copy(place).start()
    quantized, coefficient = [], []
    for e in range(experts):
        scale = CLIP_RATIO * (peak_ref[e : e + 1] + EPSILON) / 127.0
        inverse = column_of(1.0 / scale)[:, 0:1]
        quantized.append(jnp.clip(hidden_ref[e] * inverse, -127.0, 127.0).astype(jnp.bfloat16))
        coefficient.append(column_of(scale * share_ref[e : e + 1]))
    place = 0
    for offsets, ref in zip(outputs, out_refs):
        for b in range(len(offsets)):
            copy(place).wait()
            total = None
            for e in range(experts):
                acc = jnp.dot(quantized[e], weights[place, e], preferred_element_type=jnp.float32)
                term = acc * coefficient[e] * ds_ref[e : e + 1, columns(place)]
                total = term if total is None else total + term
            if from_ref is not None:
                total = total + from_ref[place].astype(jnp.float32)
            ref[b] = total.astype(ref.dtype)
            place += 1


def down(me, hidden, peaks, share, w_down, down_scale, outputs, types, arrived, n):
    experts, rows, units = hidden.shape
    vmem = pl.BlockSpec(memory_space=pltpu.VMEM)
    extra = [] if arrived is None else [arrived]
    count = sum(map(len, outputs))
    return pl.pallas_call(
        functools.partial(down_kernel, outputs, n),
        out_shape=tuple(
            jax.ShapeDtypeStruct((len(o), rows, LANES), t) for o, t in zip(outputs, types)
        ),
        in_specs=[pl.BlockSpec(memory_space=pltpu.SMEM)]
        + [vmem] * 4
        + [pl.BlockSpec(memory_space=pltpu.HBM)]
        + [vmem] * len(extra),
        out_specs=tuple(vmem for _ in outputs),
        scratch_shapes=[
            pltpu.VMEM((count, experts, units, LANES), w_down.dtype),
            pltpu.SemaphoreType.DMA((count,)),
        ],
        compiler_params=pltpu.CompilerParams(vmem_limit_bytes=32 << 20),
        cost_estimate=pl.CostEstimate(
            flops=4 * rows * units * n * LANES, bytes_accessed=8 << 20, transcendentals=0
        ),
        name="down",
    )(
        me, hidden, peaks, share, down_scale, pltpu.with_memory_space_constraint(w_down, pltpu.HBM), *extra
    )


def peaks_of_all(peaks):
    size = lax.axis_size("tp")
    near = [list(range(i, i + STRIDE)) for i in range(0, size, STRIDE)]
    copies = jnp.broadcast_to(peaks[None], (STRIDE, *peaks.shape))
    peaks = lax.all_to_all(copies, "tp", 0, 0, axis_index_groups=near, tiled=True).max(axis=0)
    return lax.pmax(lax.optimization_barrier(peaks), "tp", axis_index_groups=strided_groups(size))


def sum_over_tp(up, down_, base):
    def wide(a):
        return a.astype(jnp.float32)

    def sent(a):
        return a.astype(jnp.bfloat16)

    u, v = shift(up[0], 1), shift(down_[0], -1)
    u2, v2 = shift(up[1], 1), shift(down_[1], -1)
    outer = jnp.concatenate([base[:1] + wide(u[:1]), base[1:OUTER] + wide(u[1:]) + wide(v)])
    plus, minus = both_ways(sent(outer[1]), sent(outer[0]), 3)
    plus, minus = both_ways(sent(outer[3] + wide(plus)), sent(outer[2] + wide(minus)), 3)
    inner = base[OUTER:] + wide(u2) + wide(v2)
    for i in range(0, inner.shape[0] - 1, 2):
        plus, minus = both_ways(sent(inner[i + 1] + wide(plus)), sent(inner[i] + wide(minus)), 3)
    return (inner[-1] + wide(plus) + wide(minus)).astype(jnp.bfloat16)


def per_device(
    tokens,
    smooth_in,
    expert_ids,
    gate_fixed,
    slots,
    w_gate,
    w_up,
    w_down,
    gate_scale,
    up_scale,
    smooth_mid,
    down_scale,
):
    local_experts = w_gate.shape[0]
    rows = tokens.shape[0]
    capacity = 3 * rows // 4
    group = lax.axis_index("exp")
    n = lax.axis_size("tp")
    assert n == 32 and tokens.shape[1] == LANES
    me = lax.axis_index("tp").astype(jnp.int32).reshape(1)

    packed = pack(tokens, smooth_in)
    q, scale = quantize(me, gather_features(packed), rows, n)

    gate_values = gate_fixed.astype(jnp.float32)
    weight = gate_values / jnp.sum(gate_values, axis=1, keepdims=True)
    pair_weight = jnp.where(slots < capacity, weight, 0.0)

    def shares_of(which):
        experts = which * local_experts + jnp.arange(local_experts, dtype=jnp.int32)
        hit = expert_ids[:, :, None] == experts[None, None, :]
        return jnp.sum(jnp.where(hit, pair_weight[:, :, None], 0.0), axis=1).T

    share = shares_of(group)
    notes = jnp.concatenate([shares_of(1 - group), scale[: 8 - local_experts]])
    other_q = to_partner(q)
    other_notes = to_partner(notes)
    other_share, other_scale = other_notes[:local_experts], other_notes[local_experts : local_experts + 1]

    weights = (
        jnp.swapaxes(w_gate, 1, 2), jnp.swapaxes(w_up, 1, 2), gate_scale, up_scale, smooth_mid,
    )
    hidden, peak = hidden_of(q, scale[:1], *weights)
    other_hidden, other_peak = hidden_of(other_q, other_scale, *weights)
    peaks = peaks_of_all(jnp.concatenate([peak[:, 0], other_peak[:, 0]]))

    outputs = (SUM_UP[:OUTER], SUM_DOWN[: OUTER - 1], SUM_UP[OUTER:], SUM_DOWN[OUTER - 1 :], SUM_BASE)
    order = (sum(outputs, ()),)
    (other_part,) = down(
        me, other_hidden, peaks[local_experts:], other_share, w_down, down_scale,
        order, (jnp.bfloat16,), None, n,
    )
    arrived = to_partner(other_part)
    types = (jnp.bfloat16,) * 4 + (jnp.float32,)
    partial = down(
        me, hidden, peaks[:local_experts], share, w_down, down_scale, outputs, types, arrived, n
    )
    return sum_over_tp(partial[0:3:2], partial[1:4:2], partial[4])


def solution(mesh):
    in_specs = (
        P(("rep", "exp"), "tp"),
        P("tp"),
        P(("rep", "exp"), None),
        P(("rep", "exp"), None),
        P(("rep", "exp"), None),
        P("exp", None, "tp"),
        P("exp", None, "tp"),
        P("exp", "tp", None),
        P("exp", "tp"),
        P("exp", "tp"),
        P("exp", "tp"),
        P("exp", None),
    )
    out_specs = P(("rep", "exp"), "tp")
    return jax.shard_map(
        per_device, mesh=mesh, in_specs=in_specs, out_specs=out_specs, check_vma=False
    )
```

```python
import functools

import jax
import jax.numpy as jnp
from jax import lax
from jax.experimental import pallas as pl
from jax.experimental.pallas import tpu as pltpu
from jax.sharding import PartitionSpec as P

CLIP_RATIO = 0.35
EPSILON = 1e-06
LANES = 128
PAD = 8

SUM_BASE = (-15, 15, -12, 12, -9, 9, -6, 6, -3, 3, 0)
OUTER = 4
SUM_UP = tuple(o + 1 for o in SUM_BASE)
SUM_DOWN = tuple(o - 1 for o in SUM_BASE[1:])
STRIDE = 4


def split_three(value):
    high = lax.reduce_precision(value, 8, 7)
    rest = value - high
    middle = lax.reduce_precision(rest, 8, 7)
    low = lax.reduce_precision(rest - middle, 8, 7)
    return high, middle, low


def to_partner(array):
    return lax.ppermute(array, "exp", [(0, 1), (1, 0)])


def shift(array, by):
    size = lax.axis_size("tp")
    return lax.ppermute(array, "tp", [(i, (i + by) % size) for i in range(size)])


def both_ways(up, down, by):
    return lax.optimization_barrier((shift(up, by), shift(down, -by)))


def strided_groups(size):
    return [list(range(i, size, STRIDE)) for i in range(STRIDE)]


def gather_features(packed):
    groups = strided_groups(lax.axis_size("tp"))
    count = len(groups[0])
    base = lax.all_gather(packed, "tp", axis=0, axis_index_groups=groups)
    base = lax.optimization_barrier(base)
    left, right = both_ways(base, base, 1)
    left2, right2 = both_ways(left[: count // 2], right[count // 2 :], 1)
    return ((base, 0, 0), (left, -1, 0), (right, 1, 0), (left2, -2, 0), (right2, 2, count // 2))


def column_of(row):
    return jnp.transpose(jnp.broadcast_to(row, (LANES, row.shape[1])))


def row_of(column):
    return jnp.transpose(jnp.broadcast_to(column, (column.shape[0], LANES)))[0:1]


def quantize_kernel(places, n, me_ref, *refs):
    blocks, (q_ref, scale_ref) = refs[: len(places)], refs[len(places) :]
    rows = q_ref.shape[0]
    me = me_ref[0]

    def smoothed(ref, b):
        values = ref[b].astype(jnp.float32)
        factor = values[rows : rows + 1] + values[rows + 1 : rows + 2] + values[rows + 2 : rows + 3]
        return values[:rows] * (1.0 / factor)

    peak = jnp.zeros((rows, LANES), jnp.float32)
    for ref in blocks:
        for b in range(ref.shape[0]):
            peak = jnp.maximum(peak, jnp.abs(smoothed(ref, b)))
    scale = CLIP_RATIO * (jnp.max(peak, axis=1, keepdims=True) + EPSILON) / 127.0
    scale_ref[...] = jnp.broadcast_to(row_of(scale), scale_ref.shape)
    inverse = 1.0 / scale
    for ref, (step, first) in zip(blocks, places):
        column = lax.rem(me + (step + n), STRIDE)
        for b in range(ref.shape[0]):
            start = pl.multiple_of((column + STRIDE * (first + b)) * LANES, LANES)
            value = jnp.clip(smoothed(ref, b) * inverse, -127.0, 127.0)
            q_ref[:, pl.ds(start, LANES)] = value.astype(jnp.bfloat16)


def quantize(me, gathered, rows, n):
    arrays = [array for array, _, _ in gathered]
    places = [(step, first) for _, step, first in gathered]
    vmem = pl.BlockSpec(memory_space=pltpu.VMEM)
    return pl.pallas_call(
        functools.partial(quantize_kernel, places, n),
        out_shape=(
            jax.ShapeDtypeStruct((rows, n * LANES), jnp.bfloat16),
            jax.ShapeDtypeStruct((8, rows), jnp.float32),
        ),
        in_specs=[pl.BlockSpec(memory_space=pltpu.SMEM)] + [vmem] * len(arrays),
        out_specs=(vmem, vmem),
        compiler_params=pltpu.CompilerParams(vmem_limit_bytes=24 << 20),
        cost_estimate=pl.CostEstimate(flops=20_000_000, bytes_accessed=4 << 20, transcendentals=0),
        name="quantize",
    )(me, *arrays)


def hidden_kernel(q_ref, scale_ref, gate_ref, up_ref, gs_ref, us_ref, sm_ref, hidden_ref, peak_ref):
    scale = column_of(scale_ref[...])[:, 0:1]
    contract = (((1,), (1,)), ((), ()))
    gate = lax.dot_general(q_ref[...], gate_ref[0], contract, preferred_element_type=jnp.float32)
    up = lax.dot_general(q_ref[...], up_ref[0], contract, preferred_element_type=jnp.float32)
    gate = gate * scale * gs_ref[0]
    up = up * scale * us_ref[0]
    hidden = gate * (1.0 / (1.0 + jnp.exp(-gate))) * up * (1.0 / sm_ref[0])
    hidden_ref[0] = hidden
    peak_ref[0] = row_of(jnp.max(jnp.abs(hidden), axis=1, keepdims=True))


def hidden_of(q, scale, gate_t, up_t, gate_scale, up_scale, smooth_mid):
    experts, units, depth = gate_t.shape
    rows = q.shape[0]
    weights = pl.BlockSpec((1, units, depth), lambda e: (e, 0, 0))
    channel = pl.BlockSpec((1, 1, units), lambda e: (e, 0, 0))
    return pl.pallas_call(
        hidden_kernel,
        grid=(experts,),
        out_shape=(
            jax.ShapeDtypeStruct((experts, rows, units), jnp.float32),
            jax.ShapeDtypeStruct((experts, 1, rows), jnp.float32),
        ),
        in_specs=[
            pl.BlockSpec((rows, depth), lambda e: (0, 0)),
            pl.BlockSpec((1, rows), lambda e: (0, 0)),
            weights, weights, channel, channel, channel,
        ],
        out_specs=(
            pl.BlockSpec((1, rows, units), lambda e: (e, 0, 0)),
            pl.BlockSpec((1, 1, rows), lambda e: (e, 0, 0)),
        ),
        compiler_params=pltpu.CompilerParams(vmem_limit_bytes=24 << 20),
        cost_estimate=pl.CostEstimate(
            flops=4 * experts * rows * units * depth, bytes_accessed=10 << 20, transcendentals=0
        ),
        name="hidden",
    )(q, scale, gate_t, up_t, gate_scale[:, None], up_scale[:, None], smooth_mid[:, None])


def down_kernel(outputs, n, me_ref, hidden_ref, peak_ref, share_ref, down_ref, ds_ref, *refs):
    out_refs = refs[-len(outputs) :]
    from_ref = refs[0] if len(refs) > len(outputs) else None
    experts = hidden_ref.shape[0]
    me = me_ref[0]
    quantized, coefficient = [], []
    for e in range(experts):
        scale = CLIP_RATIO * (peak_ref[e : e + 1] + EPSILON) / 127.0
        inverse = column_of(1.0 / scale)[:, 0:1]
        quantized.append(jnp.clip(hidden_ref[e] * inverse, -127.0, 127.0).astype(jnp.bfloat16))
        coefficient.append(column_of(scale * share_ref[e : e + 1]))
    place = 0
    for offsets, ref in zip(outputs, out_refs):
        for b, offset in enumerate(offsets):
            start = pl.multiple_of(lax.rem(me + (offset + n), n) * LANES, LANES)
            total = None
            for e in range(experts):
                acc = jnp.dot(
                    quantized[e], down_ref[e, :, pl.ds(start, LANES)], preferred_element_type=jnp.float32
                )
                term = acc * coefficient[e] * ds_ref[e : e + 1, pl.ds(start, LANES)]
                total = term if total is None else total + term
            if from_ref is not None:
                total = total + from_ref[place].astype(jnp.float32)
            ref[b] = total.astype(ref.dtype)
            place += 1


def down(me, hidden, peaks, share, w_down, down_scale, outputs, types, arrived, n):
    rows, units = hidden.shape[1:]
    vmem = pl.BlockSpec(memory_space=pltpu.VMEM)
    extra = [] if arrived is None else [arrived]
    return pl.pallas_call(
        functools.partial(down_kernel, outputs, n),
        out_shape=tuple(
            jax.ShapeDtypeStruct((len(o), rows, LANES), t) for o, t in zip(outputs, types)
        ),
        in_specs=[pl.BlockSpec(memory_space=pltpu.SMEM)] + [vmem] * (5 + len(extra)),
        out_specs=tuple(vmem for _ in outputs),
        compiler_params=pltpu.CompilerParams(vmem_limit_bytes=32 << 20),
        cost_estimate=pl.CostEstimate(
            flops=4 * rows * units * n * LANES, bytes_accessed=8 << 20, transcendentals=0
        ),
        name="down",
    )(me, hidden, peaks, share, w_down, down_scale, *extra)


def peaks_of_all(peaks):
    size = lax.axis_size("tp")
    near = [list(range(i, i + STRIDE)) for i in range(0, size, STRIDE)]
    copies = jnp.broadcast_to(peaks[None], (STRIDE, *peaks.shape))
    peaks = lax.all_to_all(copies, "tp", 0, 0, axis_index_groups=near, tiled=True).max(axis=0)
    return lax.pmax(lax.optimization_barrier(peaks), "tp", axis_index_groups=strided_groups(size))


def sum_over_tp(up, down_, base):
    def wide(a):
        return a.astype(jnp.float32)

    def sent(a):
        return a.astype(jnp.bfloat16)

    u, v = shift(up[0], 1), shift(down_[0], -1)
    u2, v2 = shift(up[1], 1), shift(down_[1], -1)
    outer = jnp.concatenate([base[:1] + wide(u[:1]), base[1:OUTER] + wide(u[1:]) + wide(v)])
    plus, minus = both_ways(sent(outer[1]), sent(outer[0]), 3)
    plus, minus = both_ways(sent(outer[3] + wide(plus)), sent(outer[2] + wide(minus)), 3)
    inner = base[OUTER:] + wide(u2) + wide(v2)
    for i in range(0, inner.shape[0] - 1, 2):
        plus, minus = both_ways(sent(inner[i + 1] + wide(plus)), sent(inner[i] + wide(minus)), 3)
    return (inner[-1] + wide(plus) + wide(minus)).astype(jnp.bfloat16)


def per_device(
    tokens,
    smooth_in,
    expert_ids,
    gate_fixed,
    slots,
    w_gate,
    w_up,
    w_down,
    gate_scale,
    up_scale,
    smooth_mid,
    down_scale,
):
    local_experts = w_gate.shape[0]
    rows = tokens.shape[0]
    capacity = 3 * rows // 4
    group = lax.axis_index("exp")
    n = lax.axis_size("tp")
    assert n == 32 and tokens.shape[1] == LANES
    me = lax.axis_index("tp").astype(jnp.int32).reshape(1)

    parts = jnp.stack(split_three(smooth_in))
    parts = jnp.concatenate([parts, jnp.zeros((PAD - 3, LANES), parts.dtype)])
    packed = jnp.concatenate([tokens, parts.astype(jnp.bfloat16)])
    q, scale = quantize(me, gather_features(packed), rows, n)

    gate_values = gate_fixed.astype(jnp.float32)
    weight = gate_values / jnp.sum(gate_values, axis=1, keepdims=True)
    pair_weight = jnp.where(slots < capacity, weight, 0.0)

    def shares_of(which):
        experts = which * local_experts + jnp.arange(local_experts, dtype=jnp.int32)
        hit = expert_ids[:, :, None] == experts[None, None, :]
        return jnp.sum(jnp.where(hit, pair_weight[:, :, None], 0.0), axis=1).T

    share = shares_of(group)
    notes = jnp.concatenate([shares_of(1 - group), scale[: 8 - local_experts]])
    other_q = to_partner(q)
    other_notes = to_partner(notes)
    other_share, other_scale = other_notes[:local_experts], other_notes[local_experts : local_experts + 1]

    weights = (
        jnp.swapaxes(w_gate, 1, 2), jnp.swapaxes(w_up, 1, 2), gate_scale, up_scale, smooth_mid,
    )
    hidden, peak = hidden_of(q, scale[:1], *weights)
    other_hidden, other_peak = hidden_of(other_q, other_scale, *weights)
    peaks = peaks_of_all(jnp.concatenate([peak[:, 0], other_peak[:, 0]]))

    def parts(which, peak, portion, outputs, types, arrived):
        return down(me, which, peak, portion, w_down, down_scale, outputs, types, arrived, n)

    early = (SUM_UP[:OUTER], SUM_DOWN[: OUTER - 1], SUM_UP[OUTER:], SUM_DOWN[OUTER - 1 :])
    other = (other_hidden, peaks[local_experts:], other_share)
    own = (hidden, peaks[:local_experts], share)
    (first,) = parts(*other, (sum(early, ()),), (jnp.bfloat16,), None)
    first = to_partner(first)
    (second,) = parts(*other, (SUM_BASE,), (jnp.bfloat16,), None)
    second = to_partner(second)
    sides = parts(*own, early, (jnp.bfloat16,) * 4, first)
    (base,) = parts(*own, (SUM_BASE,), (jnp.float32,), second)
    return sum_over_tp(sides[0::2], sides[1::2], base)


def solution(mesh):
    in_specs = (
        P(("rep", "exp"), "tp"),
        P("tp"),
        P(("rep", "exp"), None),
        P(("rep", "exp"), None),
        P(("rep", "exp"), None),
        P("exp", None, "tp"),
        P("exp", None, "tp"),
        P("exp", "tp", None),
        P("exp", "tp"),
        P("exp", "tp"),
        P("exp", "tp"),
        P("exp", None),
    )
    out_specs = P(("rep", "exp"), "tp")
    return jax.shard_map(
        per_device, mesh=mesh, in_specs=in_specs, out_specs=out_specs, check_vma=False
    )
```

```python
import functools

import jax
import jax.numpy as jnp
from jax import lax
from jax.experimental import pallas as pl
from jax.experimental.pallas import tpu as pltpu
from jax.sharding import PartitionSpec as P

CLIP_RATIO = 0.35
EPSILON = 1e-06
LANES = 128
PAD = 8

SUM_BASE = (-15, 15, -12, 12, -9, 9, -6, 6, -3, 3, 0)
OUTER = 2
SUM_UP = tuple(o + 1 for o in SUM_BASE)
SUM_DOWN = tuple(o - 1 for o in SUM_BASE[1:])
STRIDE = 4


def split_three(value):
    high = lax.reduce_precision(value, 8, 7)
    rest = value - high
    middle = lax.reduce_precision(rest, 8, 7)
    low = lax.reduce_precision(rest - middle, 8, 7)
    return high, middle, low


def to_partner(array):
    return lax.ppermute(array, "exp", [(0, 1), (1, 0)])


def shift(array, by):
    size = lax.axis_size("tp")
    return lax.ppermute(array, "tp", [(i, (i + by) % size) for i in range(size)])


def both_ways(up, down, by):
    return lax.optimization_barrier((shift(up, by), shift(down, -by)))


def strided_groups(size):
    return [list(range(i, size, STRIDE)) for i in range(STRIDE)]


def gather_features(packed):
    groups = strided_groups(lax.axis_size("tp"))
    count = len(groups[0])
    base = lax.all_gather(packed, "tp", axis=0, axis_index_groups=groups)
    base = lax.optimization_barrier(base)
    left, right = both_ways(base, base, 1)
    left2, right2 = both_ways(left[: count // 2], right[count // 2 :], 1)
    return ((base, 0, 0), (left, -1, 0), (right, 1, 0), (left2, -2, 0), (right2, 2, count // 2))


def column_of(row):
    return jnp.transpose(jnp.broadcast_to(row, (LANES, row.shape[1])))


def row_of(column):
    return jnp.transpose(jnp.broadcast_to(column, (column.shape[0], LANES)))[0:1]


def quantize_kernel(places, n, me_ref, *refs):
    blocks, (q_ref, scale_ref) = refs[: len(places)], refs[len(places) :]
    rows = q_ref.shape[0]
    me = me_ref[0]

    def smoothed(ref, b):
        values = ref[b].astype(jnp.float32)
        factor = values[rows : rows + 1] + values[rows + 1 : rows + 2] + values[rows + 2 : rows + 3]
        return values[:rows] * (1.0 / factor)

    peak = jnp.zeros((rows, LANES), jnp.float32)
    for ref in blocks:
        for b in range(ref.shape[0]):
            peak = jnp.maximum(peak, jnp.abs(smoothed(ref, b)))
    scale = CLIP_RATIO * (jnp.max(peak, axis=1, keepdims=True) + EPSILON) / 127.0
    scale_ref[...] = jnp.broadcast_to(row_of(scale), scale_ref.shape)
    inverse = 1.0 / scale
    for ref, (step, first) in zip(blocks, places):
        column = lax.rem(me + (step + n), STRIDE)
        for b in range(ref.shape[0]):
            start = pl.multiple_of((column + STRIDE * (first + b)) * LANES, LANES)
            value = jnp.clip(smoothed(ref, b) * inverse, -127.0, 127.0)
            q_ref[:, pl.ds(start, LANES)] = value.astype(jnp.bfloat16)


def quantize(me, gathered, rows, n):
    arrays = [array for array, _, _ in gathered]
    places = [(step, first) for _, step, first in gathered]
    vmem = pl.BlockSpec(memory_space=pltpu.VMEM)
    return pl.pallas_call(
        functools.partial(quantize_kernel, places, n),
        out_shape=(
            jax.ShapeDtypeStruct((rows, n * LANES), jnp.bfloat16),
            jax.ShapeDtypeStruct((8, rows), jnp.float32),
        ),
        in_specs=[pl.BlockSpec(memory_space=pltpu.SMEM)] + [vmem] * len(arrays),
        out_specs=(vmem, vmem),
        compiler_params=pltpu.CompilerParams(vmem_limit_bytes=24 << 20),
        cost_estimate=pl.CostEstimate(flops=20_000_000, bytes_accessed=4 << 20, transcendentals=0),
        name="quantize",
    )(me, *arrays)


def hidden_kernel(q_ref, scale_ref, gate_ref, up_ref, gs_ref, us_ref, sm_ref, hidden_ref, peak_ref):
    scale = column_of(scale_ref[...])[:, 0:1]
    contract = (((1,), (1,)), ((), ()))
    gate = lax.dot_general(q_ref[...], gate_ref[0], contract, preferred_element_type=jnp.float32)
    up = lax.dot_general(q_ref[...], up_ref[0], contract, preferred_element_type=jnp.float32)
    gate = gate * scale * gs_ref[0]
    up = up * scale * us_ref[0]
    hidden = gate * (1.0 / (1.0 + jnp.exp(-gate))) * up * (1.0 / sm_ref[0])
    hidden_ref[0] = hidden
    peak_ref[0] = row_of(jnp.max(jnp.abs(hidden), axis=1, keepdims=True))


def hidden_of(q, scale, gate_t, up_t, gate_scale, up_scale, smooth_mid):
    experts, units, depth = gate_t.shape
    rows = q.shape[0]
    weights = pl.BlockSpec((1, units, depth), lambda e: (e, 0, 0))
    channel = pl.BlockSpec((1, 1, units), lambda e: (e, 0, 0))
    return pl.pallas_call(
        hidden_kernel,
        grid=(experts,),
        out_shape=(
            jax.ShapeDtypeStruct((experts, rows, units), jnp.float32),
            jax.ShapeDtypeStruct((experts, 1, rows), jnp.float32),
        ),
        in_specs=[
            pl.BlockSpec((rows, depth), lambda e: (0, 0)),
            pl.BlockSpec((1, rows), lambda e: (0, 0)),
            weights, weights, channel, channel, channel,
        ],
        out_specs=(
            pl.BlockSpec((1, rows, units), lambda e: (e, 0, 0)),
            pl.BlockSpec((1, 1, rows), lambda e: (e, 0, 0)),
        ),
        compiler_params=pltpu.CompilerParams(vmem_limit_bytes=24 << 20),
        cost_estimate=pl.CostEstimate(
            flops=4 * experts * rows * units * depth, bytes_accessed=10 << 20, transcendentals=0
        ),
        name="hidden",
    )(q, scale, gate_t, up_t, gate_scale[:, None], up_scale[:, None], smooth_mid[:, None])


def down_kernel(outputs, n, me_ref, hidden_ref, peak_ref, share_ref, down_ref, ds_ref, *refs):
    out_refs = refs[-len(outputs) :]
    from_ref = refs[0] if len(refs) > len(outputs) else None
    experts = hidden_ref.shape[0]
    me = me_ref[0]
    quantized, coefficient = [], []
    for e in range(experts):
        scale = CLIP_RATIO * (peak_ref[e : e + 1] + EPSILON) / 127.0
        inverse = column_of(1.0 / scale)[:, 0:1]
        quantized.append(jnp.clip(hidden_ref[e] * inverse, -127.0, 127.0).astype(jnp.bfloat16))
        coefficient.append(column_of(scale * share_ref[e : e + 1]))
    place = 0
    for offsets, ref in zip(outputs, out_refs):
        for b, offset in enumerate(offsets):
            start = pl.multiple_of(lax.rem(me + (offset + n), n) * LANES, LANES)
            total = None
            for e in range(experts):
                acc = jnp.dot(
                    quantized[e], down_ref[e, :, pl.ds(start, LANES)], preferred_element_type=jnp.float32
                )
                term = acc * coefficient[e] * ds_ref[e : e + 1, pl.ds(start, LANES)]
                total = term if total is None else total + term
            if from_ref is not None:
                total = total + from_ref[place].astype(jnp.float32)
            ref[b] = total.astype(ref.dtype)
            place += 1


def down(me, hidden, peaks, share, w_down, down_scale, outputs, types, arrived, n):
    rows, units = hidden.shape[1:]
    vmem = pl.BlockSpec(memory_space=pltpu.VMEM)
    extra = [] if arrived is None else [arrived]
    return pl.pallas_call(
        functools.partial(down_kernel, outputs, n),
        out_shape=tuple(
            jax.ShapeDtypeStruct((len(o), rows, LANES), t) for o, t in zip(outputs, types)
        ),
        in_specs=[pl.BlockSpec(memory_space=pltpu.SMEM)] + [vmem] * (5 + len(extra)),
        out_specs=tuple(vmem for _ in outputs),
        compiler_params=pltpu.CompilerParams(vmem_limit_bytes=32 << 20),
        cost_estimate=pl.CostEstimate(
            flops=4 * rows * units * n * LANES, bytes_accessed=8 << 20, transcendentals=0
        ),
        name="down",
    )(me, hidden, peaks, share, w_down, down_scale, *extra)


def peaks_of_all(peaks):
    size = lax.axis_size("tp")
    near = [list(range(i, i + STRIDE)) for i in range(0, size, STRIDE)]
    copies = jnp.broadcast_to(peaks[None], (STRIDE, *peaks.shape))
    peaks = lax.all_to_all(copies, "tp", 0, 0, axis_index_groups=near, tiled=True).max(axis=0)
    return lax.pmax(lax.optimization_barrier(peaks), "tp", axis_index_groups=strided_groups(size))


def sum_over_tp(up, down_, base):
    def wide(a):
        return a.astype(jnp.float32)

    def sent(a):
        return a.astype(jnp.bfloat16)

    u, v = shift(up[0], 1), shift(down_[0], -1)
    u2, v2 = shift(up[1], 1), shift(down_[1], -1)
    outer = jnp.concatenate([base[:1] + wide(u[:1]), base[1:OUTER] + wide(u[1:]) + wide(v)])
    plus, minus = both_ways(sent(outer[1]), sent(outer[0]), 3)
    for i in range(2, OUTER, 2):
        plus, minus = both_ways(sent(outer[i + 1] + wide(plus)), sent(outer[i] + wide(minus)), 3)
    inner = base[OUTER:] + wide(u2) + wide(v2)
    for i in range(0, inner.shape[0] - 1, 2):
        plus, minus = both_ways(sent(inner[i + 1] + wide(plus)), sent(inner[i] + wide(minus)), 3)
    return (inner[-1] + wide(plus) + wide(minus)).astype(jnp.bfloat16)


def per_device(
    tokens,
    smooth_in,
    expert_ids,
    gate_fixed,
    slots,
    w_gate,
    w_up,
    w_down,
    gate_scale,
    up_scale,
    smooth_mid,
    down_scale,
):
    local_experts = w_gate.shape[0]
    rows = tokens.shape[0]
    capacity = 3 * rows // 4
    group = lax.axis_index("exp")
    n = lax.axis_size("tp")
    assert n == 32 and tokens.shape[1] == LANES
    me = lax.axis_index("tp").astype(jnp.int32).reshape(1)

    parts = jnp.stack(split_three(smooth_in))
    parts = jnp.concatenate([parts, jnp.zeros((PAD - 3, LANES), parts.dtype)])
    packed = jnp.concatenate([tokens, parts.astype(jnp.bfloat16)])
    q, scale = quantize(me, gather_features(packed), rows, n)

    gate_values = gate_fixed.astype(jnp.float32)
    weight = gate_values / jnp.sum(gate_values, axis=1, keepdims=True)
    pair_weight = jnp.where(slots < capacity, weight, 0.0)

    def shares_of(which):
        experts = which * local_experts + jnp.arange(local_experts, dtype=jnp.int32)
        hit = expert_ids[:, :, None] == experts[None, None, :]
        return jnp.sum(jnp.where(hit, pair_weight[:, :, None], 0.0), axis=1).T

    share = shares_of(group)
    notes = jnp.concatenate([shares_of(1 - group), scale[: 8 - local_experts]])
    other_q = to_partner(q)
    other_notes = to_partner(notes)
    other_share, other_scale = other_notes[:local_experts], other_notes[local_experts : local_experts + 1]

    weights = (
        jnp.swapaxes(w_gate, 1, 2), jnp.swapaxes(w_up, 1, 2), gate_scale, up_scale, smooth_mid,
    )
    hidden, peak = hidden_of(q, scale[:1], *weights)
    other_hidden, other_peak = hidden_of(other_q, other_scale, *weights)
    peaks = peaks_of_all(jnp.concatenate([peak[:, 0], other_peak[:, 0]]))

    def parts(which, peak, portion, outputs, types, arrived):
        return down(me, which, peak, portion, w_down, down_scale, outputs, types, arrived, n)

    early = (SUM_UP[:OUTER], SUM_DOWN[: OUTER - 1], SUM_UP[OUTER:], SUM_DOWN[OUTER - 1 :])
    other = (other_hidden, peaks[local_experts:], other_share)
    own = (hidden, peaks[:local_experts], share)
    (first,) = parts(*other, (sum(early, ()),), (jnp.bfloat16,), None)
    first = to_partner(first)
    (second,) = parts(*other, (SUM_BASE,), (jnp.bfloat16,), None)
    second = to_partner(second)
    sides = parts(*own, early, (jnp.bfloat16,) * 4, first)
    (base,) = parts(*own, (SUM_BASE,), (jnp.float32,), second)
    return sum_over_tp(sides[0::2], sides[1::2], base)


def solution(mesh):
    in_specs = (
        P(("rep", "exp"), "tp"),
        P("tp"),
        P(("rep", "exp"), None),
        P(("rep", "exp"), None),
        P(("rep", "exp"), None),
        P("exp", None, "tp"),
        P("exp", None, "tp"),
        P("exp", "tp", None),
        P("exp", "tp"),
        P("exp", "tp"),
        P("exp", "tp"),
        P("exp", None),
    )
    out_specs = P(("rep", "exp"), "tp")
    return jax.shard_map(
        per_device, mesh=mesh, in_specs=in_specs, out_specs=out_specs, check_vma=False
    )
```
